32 devices in a mesh: ep: 32 (over z, y, x, core).
Axes of the slice: x: 2, y: 2, z: 4, core: 2. Of those that a mesh axis runs over, the one named last changes fastest.
Arguments:
- tokens: bfloat16 [192, 1024, 1024], P('ep')
- loss_weight: bfloat16 [192, 1024, 1024], P('ep')
- w_gate: bfloat16 [1024, 32], replicated
- w_in: bfloat16 [32, 1024, 512], P('ep')
- w_out: bfloat16 [32, 512, 1024], P('ep')
- first_expert: int32 [192, 1024], P('ep')
- second_expert: int32 [192, 1024], P('ep')
- keep_second: int32 [192, 1024], P('ep')
Outputs:
- output 1: float32 [], replicated
- output 2: bfloat16 [192, 1024, 1024], P('ep')
- output 3: bfloat16 [32, 1024, 512], P('ep')
- output 4: bfloat16 [32, 512, 1024], P('ep')
- output 5: float32 [1024, 32], replicated
All inputs are finite; a program needn't handle non-finite values.
Results may differ from the reference program's by a relative error of at most 0.00968334.
Values are sent between devices in bfloat16 or wider.
A program may use at most 1 GiB of HBM per device.

```python
import jax
import jax.numpy as jnp
from jax import lax

EXPERTS = 32
HIDDEN = 1024
FF_DIM = 512
SEQ_LEN = 1024
GROUPS = 192
CAPACITY = 2 * SEQ_LEN // EXPERTS
TOKENS = GROUPS * SEQ_LEN
NUMEL = TOKENS * HIDDEN
ALPHA = 0.01


def draw_routes(route_key):
    sub_keys = jax.random.split(route_key, 6)
    skew_level = jax.random.randint(sub_keys[0], (GROUPS, 1), 0, 4)
    hot_expert = jax.random.randint(sub_keys[1], (GROUPS, 1), 0, EXPERTS)
    hot_pick = jax.random.randint(sub_keys[2], (GROUPS, SEQ_LEN), 0, 8)
    spread = jax.random.randint(sub_keys[3], (GROUPS, SEQ_LEN), 0, EXPERTS)
    first_expert = jnp.where(hot_pick < skew_level, hot_expert, spread).astype(jnp.int32)
    offset = jax.random.randint(sub_keys[4], (GROUPS, SEQ_LEN), 1, EXPERTS)
    second_expert = ((first_expert + offset) % EXPERTS).astype(jnp.int32)
    keep_second = (jax.random.randint(sub_keys[5], (GROUPS, SEQ_LEN), 0, 3) > 0).astype(jnp.int32)
    return first_expert, second_expert, keep_second


def setup_inputs(seed: int = 0) -> dict:
    sub_keys = jax.random.split(jax.random.key(seed), 6)
    tokens = jax.random.normal(sub_keys[0], (GROUPS, SEQ_LEN, HIDDEN), jnp.float32).astype(jnp.bfloat16)
    loss_weight = jax.random.normal(sub_keys[1], (GROUPS, SEQ_LEN, HIDDEN), jnp.float32).astype(jnp.bfloat16)
    w_gate = (jax.random.normal(sub_keys[2], (HIDDEN, EXPERTS), jnp.float32) * HIDDEN ** -0.5).astype(jnp.bfloat16)
    w_in = (jax.random.normal(sub_keys[3], (EXPERTS, HIDDEN, FF_DIM), jnp.float32) * HIDDEN ** -0.5).astype(jnp.bfloat16)
    w_out = (jax.random.normal(sub_keys[4], (EXPERTS, FF_DIM, HIDDEN), jnp.float32) * FF_DIM ** -0.5).astype(jnp.bfloat16)
    first_expert, second_expert, keep_second = draw_routes(sub_keys[5])
    return {'tokens': tokens, 'loss_weight': loss_weight, 'w_gate': w_gate, 'w_in': w_in, 'w_out': w_out, 'first_expert': first_expert, 'second_expert': second_expert, 'keep_second': keep_second}


def table_for(hot_rows, pos_rows, kept_rows):
    slot_ids = jnp.arange(CAPACITY, dtype=jnp.int32)
    slot_hit = ((pos_rows[:, None, None] == slot_ids) & (kept_rows[:, None, None] > 0)).astype(jnp.float32)
    return hot_rows[:, :, None] * slot_hit


def expert_apply(packed):
    x_slots, w_first, w_second = packed
    pre_act = jnp.einsum('gch,hf->gcf', x_slots.astype(jnp.float32), w_first.astype(jnp.float32))
    act_bf = jax.nn.gelu(pre_act, approximate=True).astype(jnp.bfloat16)
    return jnp.einsum('gcf,fh->gch', act_bf.astype(jnp.float32), w_second.astype(jnp.float32)).astype(jnp.bfloat16)


def reference(tokens, loss_weight, w_gate, w_in, w_out, first_expert, second_expert, keep_second):
    expert_ids = jnp.arange(EXPERTS, dtype=jnp.int32)
    first_int = (first_expert[..., None] == expert_ids).astype(jnp.int32)
    second_int = (second_expert[..., None] == expert_ids).astype(jnp.int32)
    second_keep = second_int * keep_second[..., None]
    first_count = jnp.sum(first_int, axis=1)
    pos_first = jnp.sum((jnp.cumsum(first_int, axis=1) - first_int) * first_int, axis=-1)
    pos_second = jnp.sum((jnp.cumsum(second_keep, axis=1) - second_keep + first_count[:, None, :]) * second_int, axis=-1)
    kept_first = (pos_first < CAPACITY).astype(jnp.int32)
    kept_second = keep_second * (pos_second < CAPACITY).astype(jnp.int32)
    first_hot = first_int.astype(jnp.float32)
    second_hot = second_int.astype(jnp.float32)
    frac_first = jnp.sum(first_hot, axis=(0, 1)) / TOKENS

    def dispatch_group(packed):
        x_group, pos_one, kept_one, hot_one, pos_two, kept_two, hot_two = packed
        table = table_for(hot_one, pos_one, kept_one) + table_for(hot_two, pos_two, kept_two)
        return jnp.einsum('sec,sh->ech', table, x_group).astype(jnp.bfloat16)

    def combine_group(packed):
        y_group, pos_one, kept_one, hot_one, pos_two, kept_two, hot_two, norm_one, norm_two = packed
        combine = (table_for(hot_one, pos_one, kept_one) * norm_one[:, None, None] + table_for(hot_two, pos_two, kept_two) * norm_two[:, None, None]).astype(jnp.bfloat16)
        return jnp.einsum('sec,ech->sh', combine.astype(jnp.float32), y_group.astype(jnp.float32))

    def objective(x_in, gate_w, w_first, w_second):
        x_f32 = x_in.astype(jnp.float32)
        logits = jnp.einsum('gsh,he->gse', x_f32, gate_w)
        router_prob = jax.nn.softmax(logits, axis=-1)
        gate_first = jnp.sum(router_prob * first_hot, axis=-1)
        gate_second = jnp.sum(router_prob * second_hot, axis=-1)
        norm_first = gate_first / (gate_first + gate_second)
        norm_second = gate_second / (gate_first + gate_second)
        slots_in = lax.map(jax.checkpoint(dispatch_group), (x_f32, pos_first, kept_first, first_hot, pos_second, kept_second, second_hot))
        slots_out = lax.map(jax.checkpoint(expert_apply), (jnp.moveaxis(slots_in, 0, 1), w_first, w_second))
        moe_out = lax.map(jax.checkpoint(combine_group), (jnp.moveaxis(slots_out, 0, 1), pos_first, kept_first, first_hot, pos_second, kept_second, second_hot, norm_first, norm_second))
        dot_sum = jnp.sum((x_f32 + moe_out) * loss_weight.astype(jnp.float32))
        mean_prob = jnp.sum(router_prob, axis=(0, 1)) / TOKENS
        loss_value = dot_sum / NUMEL + ALPHA * EXPERTS * jnp.sum(frac_first * mean_prob)
        return loss_value * NUMEL, loss_value

    _, pull_back, loss_value = jax.vjp(objective, tokens, w_gate.astype(jnp.float32), w_in, w_out, has_aux=True)
    grad_x, grad_gate, grad_w_in, grad_w_out = pull_back(jnp.ones((), jnp.float32))
    return loss_value, grad_x, grad_w_in, grad_w_out, grad_gate
```

```python
import jax
import jax.numpy as jnp
from jax import lax
from jax.sharding import PartitionSpec as P

ALPHA = 0.01
CHUNKS = 2
F32 = jnp.float32
BF16 = jnp.bfloat16


def gelu_bf16(pre_act):
    return jax.nn.gelu(pre_act, approximate=True).astype(BF16)


def slot_numbers(first_ids, second_ids, keep_ids, experts, cap_rows):
    seq_len = first_ids.shape[1]
    expert_ids = jnp.arange(experts, dtype=jnp.int32)
    first_hot = (first_ids[..., None] == expert_ids).astype(BF16)
    second_hot = (second_ids[..., None] == expert_ids).astype(BF16)
    second_kept = second_hot * keep_ids.astype(BF16)[..., None]
    seq_ids = jnp.arange(seq_len, dtype=jnp.int32)
    earlier = (seq_ids[:, None] > seq_ids[None, :]).astype(BF16)
    before_first = jnp.einsum('st,gte->gse', earlier, first_hot, preferred_element_type=F32)
    before_second = jnp.einsum('st,gte->gse', earlier, second_kept, preferred_element_type=F32)
    first_count = jnp.sum(first_hot, axis=1, dtype=F32)
    pos_first = jnp.sum(before_first * first_hot, axis=-1).astype(jnp.int32)
    pos_second = jnp.sum((before_second + first_count[:, None, :]) * second_hot, axis=-1).astype(jnp.int32)
    pos_first = jnp.where(pos_first < cap_rows, pos_first, -1)
    pos_second = jnp.where((keep_ids > 0) & (pos_second < cap_rows), pos_second, -1)
    return first_hot, second_hot, first_count, pos_first, pos_second


def solution(mesh):
    ep_size = mesh.shape['ep']

    def layer_body(x_loc, r_loc, w_gate, w_in_loc, w_out_loc, first_ids, second_ids, keep_ids):
        local_groups, seq_len, hidden = x_loc.shape
        experts = w_gate.shape[1]
        ff_dim = w_in_loc.shape[2]
        cap_rows = 2 * seq_len // experts
        tokens_all = local_groups * ep_size * seq_len
        numel = tokens_all * hidden
        part = ff_dim // CHUNKS

        w_in_parts = [lax.all_gather(w_in_loc[:, :, c * part:(c + 1) * part], 'ep', axis=0, tiled=True) for c in range(CHUNKS)]
        w_out_parts = [lax.all_gather(w_out_loc[:, c * part:(c + 1) * part, :], 'ep', axis=0, tiled=True) for c in range(CHUNKS)]

        first_hot, second_hot, first_count, pos_first, pos_second = slot_numbers(first_ids, second_ids, keep_ids, experts, cap_rows)
        logits = jnp.einsum('gsh,he->gse', x_loc, w_gate, preferred_element_type=F32)
        router_prob = jax.nn.softmax(logits, axis=-1)
        gate_first = jnp.sum(router_prob * first_hot, axis=-1)
        gate_second = jnp.sum(router_prob * second_hot, axis=-1)
        gate_sum = gate_first + gate_second
        norm_first = (gate_first / gate_sum).astype(BF16)
        norm_second = (gate_second / gate_sum).astype(BF16)
        slot_ids = jnp.arange(cap_rows, dtype=jnp.int32)
        place_first = (pos_first[..., None] == slot_ids).astype(BF16)
        place_second = (pos_second[..., None] == slot_ids).astype(BF16)
        flat_first = jnp.where(pos_first >= 0, first_ids * cap_rows + pos_first, -1)
        flat_second = jnp.where(pos_second >= 0, second_ids * cap_rows + pos_second, -1)
        flat_ids = jnp.arange(experts * cap_rows, dtype=jnp.int32)
        dispatch = ((flat_first[..., None] == flat_ids) | (flat_second[..., None] == flat_ids)).astype(BF16)
        norm_slots = (jnp.einsum('gse,gsc->gec', first_hot * norm_first[..., None], place_first, preferred_element_type=F32)
                      + jnp.einsum('gse,gsc->gec', second_hot * norm_second[..., None], place_second, preferred_element_type=F32))
        slots_x = jnp.einsum('gsk,gsh->gkh', dispatch, x_loc, preferred_element_type=F32).astype(BF16)
        slots_r = jnp.einsum('gsk,gsh->gkh', dispatch, r_loc, preferred_element_type=F32)
        slots_x = slots_x.reshape(local_groups, experts, cap_rows, hidden)
        slots_r = slots_r.reshape(local_groups, experts, cap_rows, hidden)
        grad_y = (slots_r * norm_slots[..., None]).astype(BF16)
        slots_r = slots_r.astype(BF16)
        slots_x, grad_y, slots_r = (jnp.swapaxes(t, 0, 1).reshape(experts, local_groups * cap_rows, hidden) for t in (slots_x, grad_y, slots_r))

        expert_y = 0.0
        grad_slots = 0.0
        grads_in = []
        grads_out = []
        for c in range(CHUNKS):
            w_in, w_out = w_in_parts[c], w_out_parts[c]
            pre_act = jnp.einsum('emh,ehf->emf', slots_x, w_in, preferred_element_type=F32)
            act_bf, act_pull = jax.vjp(gelu_bf16, pre_act)
            grad_act = jnp.einsum('emh,efh->emf', grad_y, w_out, preferred_element_type=F32).astype(BF16)
            grad_pre = act_pull(grad_act)[0].astype(BF16)
            d_out = jnp.einsum('emf,emh->efh', act_bf, grad_y, preferred_element_type=F32)
            d_in = jnp.einsum('emh,emf->ehf', slots_x, grad_pre, preferred_element_type=F32)
            grads_out.append(lax.psum_scatter(d_out, 'ep', scatter_dimension=0, tiled=True).astype(BF16))
            grads_in.append(lax.psum_scatter(d_in, 'ep', scatter_dimension=0, tiled=True).astype(BF16))
            expert_y = expert_y + jnp.einsum('emf,efh->emh', act_bf, w_out, preferred_element_type=F32)
            grad_slots = grad_slots + jnp.einsum('emf,ehf->emh', grad_pre, w_in, preferred_element_type=F32)
        grad_w_in = jnp.concatenate(grads_in, axis=2)
        grad_w_out = jnp.concatenate(grads_out, axis=1)
        expert_y = expert_y.astype(BF16)
        grad_slots = jnp.swapaxes(grad_slots.astype(BF16).reshape(experts, local_groups, cap_rows, hidden), 0, 1).reshape(local_groups, experts * cap_rows, hidden)

        dot_slots = jnp.einsum('emh,emh->em', expert_y, slots_r, preferred_element_type=F32)
        dot_slots = jnp.swapaxes(dot_slots.reshape(experts, local_groups, cap_rows), 0, 1)
        dot_sum = jnp.einsum('gsh,gsh->', x_loc, r_loc, preferred_element_type=F32) + jnp.sum(dot_slots * norm_slots)
        local_stats = jnp.concatenate([jnp.sum(router_prob, axis=(0, 1)), dot_sum[None]])
        frac_first = lax.psum(jnp.sum(first_count, axis=0), 'ep') / tokens_all
        global_stats = lax.psum(local_stats, 'ep')
        mean_prob = global_stats[:experts] / tokens_all
        loss_value = global_stats[experts] / numel + ALPHA * experts * jnp.sum(frac_first * mean_prob)

        dot_bf = dot_slots.astype(BF16)
        grad_norm_first = jnp.sum(jnp.einsum('gse,gec->gsc', first_hot, dot_bf, preferred_element_type=F32) * place_first, axis=-1)
        grad_norm_second = jnp.sum(jnp.einsum('gse,gec->gsc', second_hot, dot_bf, preferred_element_type=F32) * place_second, axis=-1)
        gate_sq = gate_sum * gate_sum
        grad_gate_first = (grad_norm_first - grad_norm_second) * gate_second / gate_sq
        grad_gate_second = (grad_norm_second - grad_norm_first) * gate_first / gate_sq
        grad_prob = grad_gate_first[..., None] * first_hot + grad_gate_second[..., None] * second_hot + (ALPHA * hidden * experts) * frac_first
        grad_logits = router_prob * (grad_prob - jnp.sum(router_prob * grad_prob, axis=-1, keepdims=True))
        grad_logits_bf = grad_logits.astype(BF16)
        grad_x_moe = jnp.einsum('gsk,gkh->gsh', dispatch, grad_slots, preferred_element_type=F32)
        grad_x_router = jnp.einsum('gse,he->gsh', grad_logits_bf, w_gate, preferred_element_type=F32)
        grad_x = (r_loc.astype(F32) + grad_x_moe + grad_x_router).astype(BF16)
        grad_gate_w = lax.psum(jnp.einsum('gsh,gse->he', x_loc, grad_logits_bf, preferred_element_type=F32), 'ep')
        return loss_value, grad_x, grad_w_in, grad_w_out, grad_gate_w

    row_spec = P('ep', None, None)
    id_spec = P('ep', None)
    return jax.shard_map(layer_body, mesh=mesh, in_specs=(row_spec, row_spec, P(None, None), row_spec, row_spec, id_spec, id_spec, id_spec), out_specs=(P(), row_spec, row_spec, row_spec, P(None, None)), check_vma=False)
```

```python
import jax
import jax.numpy as jnp
from jax import lax
from jax.experimental import pallas as pl
from jax.experimental.pallas import tpu as pltpu
from jax.sharding import PartitionSpec as P


ALPHA = 0.01
F32 = jnp.float32
BF16 = jnp.bfloat16
I32 = jnp.int32
PLANE = 8
CHUNKS = 2
VMEM_LIMIT = 60 * 1024 * 1024


def route_slots(first_ids, second_ids, keep_ids, experts, cap_rows):
    seq_len = first_ids.shape[1]
    expert_ids = jnp.arange(experts, dtype=I32)
    first_hot = (first_ids[..., None] == expert_ids).astype(BF16)
    second_hot = (second_ids[..., None] == expert_ids).astype(BF16)
    second_kept = second_hot * keep_ids.astype(BF16)[..., None]
    seq_ids = jnp.arange(seq_len, dtype=I32)
    earlier = (seq_ids[:, None] > seq_ids[None, :]).astype(BF16)
    before_first = jnp.einsum('st,gte->gse', earlier, first_hot, preferred_element_type=F32)
    before_second = jnp.einsum('st,gte->gse', earlier, second_kept, preferred_element_type=F32)
    first_count = jnp.sum(first_hot, axis=1, dtype=F32)
    pos_first = jnp.sum(before_first * first_hot, axis=-1).astype(I32)
    pos_second = jnp.sum((before_second + first_count[:, None, :]) * second_hot, axis=-1).astype(I32)
    pos_first = jnp.where(pos_first < cap_rows, pos_first, -1)
    pos_second = jnp.where((keep_ids > 0) & (pos_second < cap_rows), pos_second, -1)
    return first_hot, second_hot, first_count, pos_first, pos_second


def dispatch_kernel(first_ref, second_ref, rows_ref, out_ref):
    peers, parts, _, cap_rows, hidden = out_ref.shape
    per_peer = parts * cap_rows
    rows = rows_ref[0]

    @pl.loop(0, peers, step=2)
    def _(peer):
        slot = lax.broadcasted_iota(I32, (2 * per_peer, rows.shape[0]), 0) + peer * per_peer
        hit = (slot == first_ref[0]) | (slot == second_ref[0])
        table = jnp.where(hit, 1.0, 0.0).astype(BF16)
        picked = jnp.dot(table, rows, preferred_element_type=F32).astype(BF16)
        out_ref[pl.ds(peer, 2)] = picked.reshape(2, parts, 1, cap_rows, hidden)


def dispatch(first_slot, second_slot, rows, parts, cap_rows):
    groups, seq_len, hidden = rows.shape
    slots = PLANE * parts * cap_rows
    return pl.pallas_call(
        dispatch_kernel,
        grid=(groups,),
        in_specs=[
            pl.BlockSpec((1, 1, seq_len), lambda g: (g, 0, 0)),
            pl.BlockSpec((1, 1, seq_len), lambda g: (g, 0, 0)),
            pl.BlockSpec((1, seq_len, hidden), lambda g: (g, 0, 0)),
        ],
        out_specs=pl.BlockSpec((PLANE, parts, 1, cap_rows, hidden), lambda g: (0, 0, g, 0, 0)),
        out_shape=jax.ShapeDtypeStruct((PLANE, parts, groups, cap_rows, hidden), BF16),
        compiler_params=pltpu.CompilerParams(vmem_limit_bytes=VMEM_LIMIT),
        cost_estimate=pl.CostEstimate(flops=2 * groups * slots * seq_len * hidden, bytes_accessed=4 * groups * seq_len * hidden, transcendentals=0),
        name='dispatch_rows',
    )(first_slot[:, None, :], second_slot[:, None, :], rows)


def dot_nn(a, b):
    return jnp.dot(a, b, preferred_element_type=F32)


def dot_nt(a, b):
    return lax.dot_general(a, b, (((1,), (1,)), ((), ())), preferred_element_type=F32)


def dot_tn(a, b):
    return lax.dot_general(a, b, (((0,), (0,)), ((), ())), preferred_element_type=F32)


def expert_kernel(x_ref, r_ref, norm_ref, w_in_ref, w_out_ref, *refs):
    slots_ref, dots_ref, d_in_ref, d_out_ref = refs[-4:]
    first = pl.program_id(1) == 0
    _, _, groups, cap_rows, hidden = x_ref.shape
    x = x_ref[...].reshape(groups * cap_rows, hidden)
    r = r_ref[...].reshape(groups * cap_rows, hidden)
    w_in = w_in_ref[0]
    w_out = w_out_ref[0]
    r_wide = r.astype(F32)
    grad_y = (r_wide * norm_ref[0, 0]).astype(BF16)
    pre = dot_nn(x, w_in)
    scale = 0.7978845608028654
    square = pre * pre
    tanh = jnp.tanh(scale * (pre + 0.044715 * (square * pre)))
    half = 0.5 * (1.0 + tanh)
    act = (pre * half).astype(BF16)
    slope = half + 0.5 * pre * (1.0 - tanh * tanh) * (scale * (1.0 + 3.0 * 0.044715 * square))
    grad_act = dot_nt(grad_y, w_out).astype(BF16).astype(F32)
    grad_pre = (grad_act * slope).astype(BF16)
    slots_ref[...] = dot_nt(grad_pre, w_in).astype(BF16).reshape(slots_ref.shape)
    out = dot_nn(act, w_out).astype(BF16).astype(F32)
    dots_ref[0, 0] = jnp.sum(out * r_wide, axis=1, keepdims=True)
    d_out = dot_tn(act, grad_y)
    d_in = dot_tn(x, grad_pre)

    @pl.when(first)
    def _():
        d_out_ref[0] = d_out
        d_in_ref[0] = d_in

    @pl.when(jnp.logical_not(first))
    def _():
        d_out_ref[0] += d_out
        d_in_ref[0] += d_in


def expert_part(part, parts, x_slots, r_slots, norms, w_in, w_out, earlier):
    peers, _, groups, cap_rows, hidden = x_slots.shape
    _, _, ff_dim = w_in.shape
    rows = groups * cap_rows
    block = pl.BlockSpec((1, 1, groups, cap_rows, hidden), lambda e, s: (s, e, 0, 0, 0))
    column = pl.BlockSpec((1, 1, rows, 1), lambda e, s: (s, e, 0, 0))
    norm_column = pl.BlockSpec((1, 1, rows, 1), lambda e, s: (s, parts * part + e, 0, 0))
    in_block = pl.BlockSpec((1, hidden, ff_dim), lambda e, s: (parts * part + e, 0, 0))
    out_block = pl.BlockSpec((1, ff_dim, hidden), lambda e, s: (parts * part + e, 0, 0))
    return pl.pallas_call(
        expert_kernel,
        grid=(parts, peers),
        in_specs=[block, block, norm_column, in_block, out_block] + [pl.BlockSpec(memory_space=pl.ANY)] * len(earlier),
        out_specs=[block, column, in_block, out_block],
        out_shape=[
            jax.ShapeDtypeStruct(x_slots.shape, BF16),
            jax.ShapeDtypeStruct((peers, parts, rows, 1), F32),
            jax.ShapeDtypeStruct(w_in.shape, F32),
            jax.ShapeDtypeStruct(w_out.shape, F32),
        ],
        input_output_aliases={5 + i: 2 + i for i in range(len(earlier))},
        compiler_params=pltpu.CompilerParams(vmem_limit_bytes=VMEM_LIMIT, dimension_semantics=('arbitrary', 'arbitrary')),
        cost_estimate=pl.CostEstimate(flops=12 * parts * peers * rows * hidden * ff_dim, bytes_accessed=6 * parts * peers * rows * hidden, transcendentals=parts * peers * rows * ff_dim),
        name='expert_part',
    )(x_slots, r_slots, norms, w_in, w_out, *earlier)


def gathered(first_ref, second_ref, slots_ref, acc):
    _, rows, _ = first_ref.shape
    slots = slots_ref[...].reshape(-1, slots_ref.shape[-1])
    slot = lax.broadcasted_iota(I32, (rows, slots.shape[0]), 1)
    hit = (slot == first_ref[0]) | (slot == second_ref[0])
    return acc + dot_nn(jnp.where(hit, 1.0, 0.0).astype(BF16), slots)


def combine_start_kernel(first_ref, second_ref, slots_ref, r_ref, logit_ref, gate_ref, out_ref):
    acc = r_ref[0].astype(F32) + dot_nn(logit_ref[0], gate_ref[...])
    out_ref[0] = gathered(first_ref, second_ref, slots_ref, acc)


def combine_more_kernel(first_ref, second_ref, slots_ref, acc_ref, out_ref):
    out_ref[0] = gathered(first_ref, second_ref, slots_ref, acc_ref[0]).astype(out_ref.dtype)


def combine(first_slot, second_slot, slots, extra, out_type):
    peers, parts, groups, cap_rows, hidden = slots.shape
    seq_len = first_slot.shape[1]
    tile = 256
    column = pl.BlockSpec((1, tile, 1), lambda g, t: (g, t, 0))
    wide = pl.BlockSpec((1, tile, hidden), lambda g, t: (g, t, 0))
    block = pl.BlockSpec((peers, parts, 1, cap_rows, hidden), lambda g, t: (0, 0, g, 0, 0))
    if len(extra) == 1:
        kernel, extra_specs = combine_more_kernel, [wide]
    else:
        experts = extra[1].shape[-1]
        kernel = combine_start_kernel
        extra_specs = [wide, pl.BlockSpec((1, tile, experts), lambda g, t: (g, t, 0)), pl.BlockSpec((experts, hidden), lambda g, t: (0, 0))]
    return pl.pallas_call(
        kernel,
        grid=(groups, seq_len // tile),
        in_specs=[column, column, block] + extra_specs,
        out_specs=wide,
        out_shape=jax.ShapeDtypeStruct((groups, seq_len, hidden), out_type),
        compiler_params=pltpu.CompilerParams(vmem_limit_bytes=VMEM_LIMIT),
        cost_estimate=pl.CostEstimate(flops=2 * groups * seq_len * peers * parts * cap_rows * hidden, bytes_accessed=10 * groups * seq_len * hidden, transcendentals=0),
        name='combine_rows',
    )(first_slot[..., None], second_slot[..., None], slots, *extra)


def after(value, *others):
    return lax.optimization_barrier((value,) + others)[0]


def solution(mesh):
    ep_size = mesh.shape['ep']
    planes = ep_size // PLANE
    plane_groups = [[z * PLANE + p for p in range(PLANE)] for z in range(planes)]
    line_groups = [[z * PLANE + p for z in range(planes)] for p in range(PLANE)]

    def swap(value):
        return lax.all_to_all(value, 'ep', 0, 0, axis_index_groups=plane_groups, tiled=True)

    def layer(x_loc, r_loc, w_gate, w_in_loc, w_out_loc, first_ids, second_ids, keep_ids):
        local_groups, seq_len, hidden = x_loc.shape
        experts = w_gate.shape[1]
        cap_rows = 2 * seq_len // experts
        tokens_all = local_groups * ep_size * seq_len
        numel = tokens_all * hidden
        parts = planes // CHUNKS

        w_in = lax.all_gather(w_in_loc, 'ep', axis=0, axis_index_groups=line_groups, tiled=True)
        w_out = lax.all_gather(w_out_loc, 'ep', axis=0, axis_index_groups=line_groups, tiled=True)

        first_hot, second_hot, first_count, pos_first, pos_second = route_slots(first_ids, second_ids, keep_ids, experts, cap_rows)

        def part_slot(ids, pos, part):
            z, peer = ids // PLANE, ids % PLANE
            here = (pos >= 0) & (z // parts == part)
            return jnp.where(here, (peer * parts + z % parts) * cap_rows + pos, -1)

        slots = [(part_slot(first_ids, pos_first, c), part_slot(second_ids, pos_second, c)) for c in range(CHUNKS)]

        def send(rows, part):
            return dispatch(*slots[part], rows, parts, cap_rows)

        sent_x = [send(x_loc, 0)]
        x_late = after(x_loc, sent_x[0])
        logits = jnp.einsum('gsh,he->gse', x_late, w_gate, preferred_element_type=F32)
        router_prob = jax.nn.softmax(logits, axis=-1)
        gate_first = jnp.sum(router_prob * first_hot, axis=-1)
        gate_second = jnp.sum(router_prob * second_hot, axis=-1)
        gate_sum = gate_first + gate_second
        norm_first = (gate_first / gate_sum).astype(BF16)
        norm_second = (gate_second / gate_sum).astype(BF16)
        slot_ids = jnp.arange(cap_rows, dtype=I32)
        place_first = (pos_first[..., None] == slot_ids).astype(BF16)
        place_second = (pos_second[..., None] == slot_ids).astype(BF16)
        norm_slots = (jnp.einsum('gse,gsc->gec', first_hot * norm_first[..., None], place_first, preferred_element_type=F32)
                      + jnp.einsum('gse,gsc->gec', second_hot * norm_second[..., None], place_second, preferred_element_type=F32))
        norm_slots = norm_slots.astype(BF16).reshape(local_groups, planes, PLANE, cap_rows).transpose(2, 1, 0, 3).reshape(PLANE, planes, local_groups * cap_rows)

        sent_r = [send(r_loc, 0)]
        got_x = [swap(sent_x[0])]
        counts = jnp.sum(first_count, axis=0)
        counts = jnp.zeros((PLANE, 1, local_groups * cap_rows), F32).at[:, :, :experts].set(counts)
        note = jnp.tile(jnp.concatenate([norm_slots.astype(F32), counts], axis=1), (planes, 1, 1))
        note = lax.all_to_all(after(note, got_x[0], sent_r[0]), 'ep', 0, 0, tiled=True)
        frac_first = jnp.sum(note[:, planes, :experts], axis=0) / tokens_all
        got_r = [swap(after(sent_r[0], note))]
        norms = lax.dynamic_slice_in_dim(note, lax.axis_index('ep') // PLANE * PLANE, PLANE, 0)[:, :planes, :, None]
        for c in range(1, CHUNKS):
            sent_x.append(send(x_late, c))
            got_x.append(swap(after(sent_x[c], got_r[c - 1])))
            sent_r.append(send(after(r_loc, sent_r[c - 1]), c))
            got_r.append(swap(after(sent_r[c], got_x[c])))
        grads = ()
        grad_slots = []
        dots = []
        for c in range(CHUNKS):
            out_slots, out_dots, *grads = expert_part(c, parts, got_x[c], got_r[c], norms, w_in, w_out, grads)
            grad_slots.append(out_slots)
            dots.append(out_dots)
        grad_w_in = lax.psum_scatter(grads[0], 'ep', scatter_dimension=0, axis_index_groups=line_groups, tiled=True).astype(BF16)
        grad_w_out = lax.psum_scatter(grads[1], 'ep', scatter_dimension=0, axis_index_groups=line_groups, tiled=True).astype(BF16)
        dots = jnp.concatenate([d[..., 0] for d in dots], axis=1)
        moe_sum = jnp.sum(dots * norms[..., 0])

        back = [swap(after(grad_slots[0], got_r[-1]))]
        dots_back = swap(after(dots.astype(BF16), back[0]))
        for c in range(1, CHUNKS):
            back.append(swap(after(grad_slots[c], dots_back if c == 1 else back[c - 1])))
        dots_back = dots_back.reshape(PLANE, planes, local_groups, cap_rows).transpose(2, 1, 0, 3).reshape(local_groups, experts, cap_rows)

        grad_norm_first = jnp.sum(jnp.einsum('gse,gec->gsc', first_hot, dots_back, preferred_element_type=F32) * place_first, axis=-1)
        grad_norm_second = jnp.sum(jnp.einsum('gse,gec->gsc', second_hot, dots_back, preferred_element_type=F32) * place_second, axis=-1)
        gate_sq = gate_sum * gate_sum
        grad_gate_first = (grad_norm_first - grad_norm_second) * gate_second / gate_sq
        grad_gate_second = (grad_norm_second - grad_norm_first) * gate_first / gate_sq
        grad_prob = grad_gate_first[..., None] * first_hot + grad_gate_second[..., None] * second_hot + (ALPHA * hidden * experts) * frac_first
        grad_logits = router_prob * (grad_prob - jnp.sum(router_prob * grad_prob, axis=-1, keepdims=True))
        grad_logits_bf = lax.optimization_barrier(grad_logits.astype(BF16))
        grad_x = combine(*slots[0], back[0], (r_loc, grad_logits_bf, w_gate.T), F32 if CHUNKS > 1 else BF16)
        for c in range(1, CHUNKS):
            grad_x = combine(*slots[c], back[c], (grad_x,), BF16 if c == CHUNKS - 1 else F32)
        grad_gate_w = jnp.einsum('gsh,gse->he', x_loc, grad_logits_bf, preferred_element_type=F32)

        dot_sum = jnp.einsum('gsh,gsh->', x_late, r_loc, preferred_element_type=F32) + moe_sum
        local_stats = jnp.concatenate([jnp.sum(router_prob, axis=(0, 1)), dot_sum[None]])
        rows = hidden * experts // ep_size // 128
        own = grad_gate_w.reshape(ep_size, rows, 128)
        shared = jnp.zeros((8, 128), F32).at[0, :experts + 1].set(local_stats)
        packed = jnp.concatenate([own, jnp.broadcast_to(shared, (ep_size, 8, 128))], axis=1)
        packed = lax.all_to_all(after(packed, back[-1]), 'ep', 0, 0, tiled=True)
        total = jnp.sum(packed, axis=0)
        grad_gate_w = lax.all_gather(total[:rows], 'ep', axis=0, tiled=True).reshape(hidden, experts)
        global_stats = total[rows]
        mean_prob = global_stats[:experts] / tokens_all
        loss_value = global_stats[experts] / numel + ALPHA * experts * jnp.sum(frac_first * mean_prob)
        return loss_value, grad_x, grad_w_in, grad_w_out, grad_gate_w

    row_spec = P('ep', None, None)
    id_spec = P('ep', None)
    return jax.shard_map(layer, mesh=mesh, in_specs=(row_spec, row_spec, P(None, None), row_spec, row_spec, id_spec, id_spec, id_spec), out_specs=(P(), row_spec, row_spec, row_spec, P(None, None)), check_vma=False)
```

```python
import jax
import jax.numpy as jnp
from jax import lax
from jax.experimental import pallas as pl
from jax.experimental.pallas import tpu as pltpu
from jax.sharding import PartitionSpec as P


ALPHA = 0.01
F32 = jnp.float32
BF16 = jnp.bfloat16
I32 = jnp.int32
PLANE = 8
LAST = 1
VMEM_LIMIT = 60 * 1024 * 1024


def route_slots(first_ids, second_ids, keep_ids, experts, cap_rows):
    seq_len = first_ids.shape[1]
    expert_ids = jnp.arange(experts, dtype=I32)
    first_hot = (first_ids[..., None] == expert_ids).astype(BF16)
    second_hot = (second_ids[..., None] == expert_ids).astype(BF16)
    second_kept = second_hot * keep_ids.astype(BF16)[..., None]
    seq_ids = jnp.arange(seq_len, dtype=I32)
    earlier = (seq_ids[:, None] > seq_ids[None, :]).astype(BF16)
    before_first = jnp.einsum('st,gte->gse', earlier, first_hot, preferred_element_type=F32)
    before_second = jnp.einsum('st,gte->gse', earlier, second_kept, preferred_element_type=F32)
    first_count = jnp.sum(first_hot, axis=1, dtype=F32)
    pos_first = jnp.sum(before_first * first_hot, axis=-1).astype(I32)
    pos_second = jnp.sum((before_second + first_count[:, None, :]) * second_hot, axis=-1).astype(I32)
    pos_first = jnp.where(pos_first < cap_rows, pos_first, -1)
    pos_second = jnp.where((keep_ids > 0) & (pos_second < cap_rows), pos_second, -1)
    return first_hot, second_hot, first_count, pos_first, pos_second


def dispatch_kernel(first_ref, second_ref, rows_ref, out_ref):
    peers, parts, _, cap_rows, hidden = out_ref.shape
    per_peer = parts * cap_rows
    rows = rows_ref[0]

    step = 4 if parts == 1 else 2

    @pl.loop(0, peers, step=step)
    def _(peer):
        slot = lax.broadcasted_iota(I32, (step * per_peer, rows.shape[0]), 0) + peer * per_peer
        hit = (slot == first_ref[0]) | (slot == second_ref[0])
        table = jnp.where(hit, 1.0, 0.0).astype(BF16)
        picked = jnp.dot(table, rows, preferred_element_type=F32).astype(BF16)
        out_ref[pl.ds(peer, step)] = picked.reshape(step, parts, 1, cap_rows, hidden)


def dispatch(first_slot, second_slot, rows, parts, cap_rows):
    groups, seq_len, hidden = rows.shape
    slots = PLANE * parts * cap_rows
    return pl.pallas_call(
        dispatch_kernel,
        grid=(groups,),
        in_specs=[
            pl.BlockSpec((1, 1, seq_len), lambda g: (g, 0, 0)),
            pl.BlockSpec((1, 1, seq_len), lambda g: (g, 0, 0)),
            pl.BlockSpec((1, seq_len, hidden), lambda g: (g, 0, 0)),
        ],
        out_specs=pl.BlockSpec((PLANE, parts, 1, cap_rows, hidden), lambda g: (0, 0, g, 0, 0)),
        out_shape=jax.ShapeDtypeStruct((PLANE, parts, groups, cap_rows, hidden), BF16),
        compiler_params=pltpu.CompilerParams(vmem_limit_bytes=VMEM_LIMIT),
        cost_estimate=pl.CostEstimate(flops=2 * groups * slots * seq_len * hidden, bytes_accessed=4 * groups * seq_len * hidden, transcendentals=0),
        name='dispatch_rows',
    )(first_slot[:, None, :], second_slot[:, None, :], rows)


def dot_nn(a, b):
    return jnp.dot(a, b, preferred_element_type=F32)


def dot_nt(a, b):
    return lax.dot_general(a, b, (((1,), (1,)), ((), ())), preferred_element_type=F32)


def dot_tn(a, b):
    return lax.dot_general(a, b, (((0,), (0,)), ((), ())), preferred_element_type=F32)


def expert_kernel(x_ref, r_ref, norm_ref, w_in_ref, w_out_ref, *refs):
    slots_ref, dots_ref, d_in_ref, d_out_ref = refs[-4:]
    first = pl.program_id(1) == 0
    _, _, groups, cap_rows, hidden = x_ref.shape
    x = x_ref[...].reshape(groups * cap_rows, hidden)
    r = r_ref[...].reshape(groups * cap_rows, hidden)
    w_in = w_in_ref[0]
    w_out = w_out_ref[0]
    r_wide = r.astype(F32)
    grad_y = (r_wide * norm_ref[0, 0]).astype(BF16)
    pre = dot_nn(x, w_in)
    scale = 0.7978845608028654
    square = pre * pre
    tanh = jnp.tanh(scale * (pre + 0.044715 * (square * pre)))
    half = 0.5 * (1.0 + tanh)
    act = (pre * half).astype(BF16)
    slope = half + 0.5 * pre * (1.0 - tanh * tanh) * (scale * (1.0 + 3.0 * 0.044715 * square))
    grad_act = dot_nt(grad_y, w_out).astype(BF16).astype(F32)
    grad_pre = (grad_act * slope).astype(BF16)
    slots_ref[...] = dot_nt(grad_pre, w_in).astype(BF16).reshape(slots_ref.shape)
    out = dot_nn(act, w_out).astype(BF16).astype(F32)
    dots_ref[0, 0] = jnp.sum(out * r_wide, axis=1, keepdims=True)
    d_out = dot_tn(act, grad_y)
    d_in = dot_tn(x, grad_pre)

    @pl.when(first)
    def _():
        d_out_ref[0] = d_out
        d_in_ref[0] = d_in

    @pl.when(jnp.logical_not(first))
    def _():
        d_out_ref[0] += d_out
        d_in_ref[0] += d_in


def expert_part(start, parts, x_slots, r_slots, norms, w_in, w_out, earlier):
    peers, _, groups, cap_rows, hidden = x_slots.shape
    _, _, ff_dim = w_in.shape
    rows = groups * cap_rows
    block = pl.BlockSpec((1, 1, groups, cap_rows, hidden), lambda e, s: (s, e, 0, 0, 0))
    column = pl.BlockSpec((1, 1, rows, 1), lambda e, s: (s, e, 0, 0))
    norm_column = pl.BlockSpec((1, 1, rows, 1), lambda e, s: (s, start + e, 0, 0))
    in_block = pl.BlockSpec((1, hidden, ff_dim), lambda e, s: (start + e, 0, 0))
    out_block = pl.BlockSpec((1, ff_dim, hidden), lambda e, s: (start + e, 0, 0))
    return pl.pallas_call(
        expert_kernel,
        grid=(parts, peers),
        in_specs=[block, block, norm_column, in_block, out_block] + [pl.BlockSpec(memory_space=pl.ANY)] * len(earlier),
        out_specs=[block, column, in_block, out_block],
        out_shape=[
            jax.ShapeDtypeStruct(x_slots.shape, BF16),
            jax.ShapeDtypeStruct((peers, parts, rows, 1), F32),
            jax.ShapeDtypeStruct(w_in.shape, F32),
            jax.ShapeDtypeStruct(w_out.shape, F32),
        ],
        input_output_aliases={5 + i: 2 + i for i in range(len(earlier))},
        compiler_params=pltpu.CompilerParams(vmem_limit_bytes=VMEM_LIMIT, dimension_semantics=('arbitrary', 'arbitrary')),
        cost_estimate=pl.CostEstimate(flops=12 * parts * peers * rows * hidden * ff_dim, bytes_accessed=6 * parts * peers * rows * hidden, transcendentals=parts * peers * rows * ff_dim),
        name='expert_part',
    )(x_slots, r_slots, norms, w_in, w_out, *earlier)


def gathered(first_ref, second_ref, slots_ref, acc):
    _, rows, _ = first_ref.shape
    slots = slots_ref[...].reshape(-1, slots_ref.shape[-1])
    slot = lax.broadcasted_iota(I32, (rows, slots.shape[0]), 1)
    hit = (slot == first_ref[0]) | (slot == second_ref[0])
    return acc + dot_nn(jnp.where(hit, 1.0, 0.0).astype(BF16), slots)


def combine_start_kernel(first_ref, second_ref, slots_ref, r_ref, out_ref):
    out_ref[0] = gathered(first_ref, second_ref, slots_ref, r_ref[0].astype(F32))


def combine_more_kernel(first_ref, second_ref, slots_ref, acc_ref, logit_ref, gate_ref, out_ref):
    acc = acc_ref[0] + dot_tn(logit_ref[0], gate_ref[...])
    out_ref[0] = gathered(first_ref, second_ref, slots_ref, acc).astype(out_ref.dtype)


def combine(first_slot, second_slot, slots, extra, out_type):
    peers, parts, groups, cap_rows, hidden = slots.shape
    seq_len = first_slot.shape[1]
    tile = 256
    column = pl.BlockSpec((1, tile, 1), lambda g, t: (g, t, 0))
    wide = pl.BlockSpec((1, tile, hidden), lambda g, t: (g, t, 0))
    block = pl.BlockSpec((peers, parts, 1, cap_rows, hidden), lambda g, t: (0, 0, g, 0, 0))
    if len(extra) == 1:
        kernel, extra_specs = combine_start_kernel, [wide]
    else:
        experts = extra[1].shape[1]
        kernel = combine_more_kernel
        extra_specs = [wide, pl.BlockSpec((1, experts, tile), lambda g, t: (g, 0, t)), pl.BlockSpec((experts, hidden), lambda g, t: (0, 0))]
    return pl.pallas_call(
        kernel,
        grid=(groups, seq_len // tile),
        in_specs=[column, column, block] + extra_specs,
        out_specs=wide,
        out_shape=jax.ShapeDtypeStruct((groups, seq_len, hidden), out_type),
        compiler_params=pltpu.CompilerParams(vmem_limit_bytes=VMEM_LIMIT),
        cost_estimate=pl.CostEstimate(flops=2 * groups * seq_len * peers * parts * cap_rows * hidden, bytes_accessed=10 * groups * seq_len * hidden, transcendentals=0),
        name='combine_rows',
    )(first_slot, second_slot, slots, *extra)


def after(value, *others):
    return lax.optimization_barrier((value,) + others)[0]


def solution(mesh):
    ep_size = mesh.shape['ep']
    planes = ep_size // PLANE
    plane_groups = [[z * PLANE + p for p in range(PLANE)] for z in range(planes)]
    line_groups = [[z * PLANE + p for z in range(planes)] for p in range(PLANE)]

    def swap(value):
        return lax.all_to_all(value, 'ep', 0, 0, axis_index_groups=plane_groups, tiled=True)

    def layer(x_loc, r_loc, w_gate, w_in_loc, w_out_loc, first_ids, second_ids, keep_ids):
        local_groups, seq_len, hidden = x_loc.shape
        experts = w_gate.shape[1]
        cap_rows = 2 * seq_len // experts
        tokens_all = local_groups * ep_size * seq_len
        numel = tokens_all * hidden
        starts = (0, planes - LAST)
        parts = (planes - LAST, LAST)

        w_in = lax.all_gather(w_in_loc, 'ep', axis=0, axis_index_groups=line_groups, tiled=True)
        w_out = lax.all_gather(w_out_loc, 'ep', axis=0, axis_index_groups=line_groups, tiled=True)

        first_hot, second_hot, first_count, pos_first, pos_second = route_slots(first_ids, second_ids, keep_ids, experts, cap_rows)

        def part_slot(ids, pos, part):
            z, peer = ids // PLANE - starts[part], ids % PLANE
            here = (pos >= 0) & (z >= 0) & (z < parts[part])
            return jnp.where(here, (peer * parts[part] + z) * cap_rows + pos, -1)

        slots = [(part_slot(first_ids, pos_first, c), part_slot(second_ids, pos_second, c)) for c in range(2)]
        columns = [(a[..., None], b[..., None]) for a, b in slots]

        def send(rows, part):
            return dispatch(*slots[part], rows, parts[part], cap_rows)

        sent_x = [send(x_loc, 0)]
        x_late = after(x_loc, sent_x[0])
        logits = jnp.einsum('gsh,he->gse', x_late, w_gate, preferred_element_type=F32)
        router_prob = jax.nn.softmax(logits, axis=-1)
        gate_first = jnp.sum(router_prob * first_hot, axis=-1)
        gate_second = jnp.sum(router_prob * second_hot, axis=-1)
        gate_sum = gate_first + gate_second
        norm_first = (gate_first / gate_sum).astype(BF16)
        norm_second = (gate_second / gate_sum).astype(BF16)
        slot_ids = jnp.arange(cap_rows, dtype=I32)
        place_first = (pos_first[..., None] == slot_ids).astype(BF16)
        place_second = (pos_second[..., None] == slot_ids).astype(BF16)
        norm_slots = (jnp.einsum('gse,gsc->gec', first_hot * norm_first[..., None], place_first, preferred_element_type=F32)
                      + jnp.einsum('gse,gsc->gec', second_hot * norm_second[..., None], place_second, preferred_element_type=F32))
        norm_slots = norm_slots.astype(BF16).reshape(local_groups, planes, PLANE, cap_rows).transpose(2, 1, 0, 3).reshape(PLANE, planes, local_groups * cap_rows)

        sent_r = [send(r_loc, 0)]
        got_x = [swap(sent_x[0])]
        counts = jnp.sum(first_count, axis=0)
        high = jnp.floor(counts / 64)
        digits = jnp.zeros((PLANE, 4, 128), BF16).at[:, 0, :experts].set(high.astype(BF16)).at[:, 1, :experts].set((counts - 64 * high).astype(BF16))
        norm_rows = planes * local_groups * cap_rows // 128
        note = jnp.tile(jnp.concatenate([norm_slots.reshape(PLANE, norm_rows, 128), digits], axis=1), (planes, 1, 1))
        note = lax.all_to_all(after(note, got_x[0], sent_r[0]), 'ep', 0, 0, tiled=True)
        digits = jnp.sum(note[:, norm_rows:norm_rows + 2, :experts].astype(F32), axis=0)
        frac_first = (64 * digits[0] + digits[1]) / tokens_all
        got_r = [swap(after(sent_r[0], note))]
        norms = lax.dynamic_slice_in_dim(note, lax.axis_index('ep') // PLANE * PLANE, PLANE, 0)[:, :norm_rows]
        norms = norms.astype(F32).reshape(PLANE, planes, local_groups * cap_rows, 1)
        plain_sum = jnp.einsum('gsh,gsh->', x_late, r_loc, preferred_element_type=F32)
        sent_x.append(send(x_late, 1))
        got_x.append(swap(after(sent_x[1], got_r[0])))
        sent_r.append(send(after(r_loc, sent_r[0]), 1))
        got_r.append(swap(after(sent_r[1], got_x[1])))
        norms, plain_sum, columns = lax.optimization_barrier((norms, plain_sum, columns))
        grads = ()
        grad_slots = []
        dots = []
        for c in range(2):
            out_slots, out_dots, *grads = expert_part(starts[c], parts[c], got_x[c], got_r[c], norms, w_in, w_out, grads)
            grad_slots.append(out_slots)
            dots.append(out_dots)
        d_in = lax.psum_scatter(grads[0], 'ep', scatter_dimension=0, axis_index_groups=line_groups, tiled=True)
        d_out = lax.psum_scatter(grads[1], 'ep', scatter_dimension=0, axis_index_groups=line_groups, tiled=True)
        grad_w_in, grad_w_out = d_in.astype(BF16), d_out.astype(BF16)
        dots = jnp.concatenate([d[..., 0] for d in dots], axis=1)
        moe_sum = jnp.sum(dots * norms[..., 0])

        back = [swap(after(grad_slots[0], got_r[-1]))]
        dots_back = swap(after(dots.astype(BF16), back[0]))
        back.append(swap(after(grad_slots[1], dots_back)))
        dots_back = dots_back.reshape(PLANE, planes, local_groups, cap_rows).transpose(2, 1, 0, 3).reshape(local_groups, experts, cap_rows)

        grad_norm_first = jnp.sum(jnp.einsum('gse,gec->gsc', first_hot, dots_back, preferred_element_type=F32) * place_first, axis=-1)
        grad_norm_second = jnp.sum(jnp.einsum('gse,gec->gsc', second_hot, dots_back, preferred_element_type=F32) * place_second, axis=-1)
        gate_sq = gate_sum * gate_sum
        grad_gate_first = (grad_norm_first - grad_norm_second) * gate_second / gate_sq
        grad_gate_second = (grad_norm_second - grad_norm_first) * gate_first / gate_sq
        grad_prob = grad_gate_first[..., None] * first_hot + grad_gate_second[..., None] * second_hot + (ALPHA * hidden * experts) * frac_first
        grad_logits = router_prob * (grad_prob - jnp.sum(router_prob * grad_prob, axis=-1, keepdims=True))
        grad_logits_bf = lax.optimization_barrier(grad_logits.astype(BF16))
        grad_x = combine(*columns[0], back[0], (r_loc,), F32)
        grad_x = combine(*columns[1], back[1], (grad_x, jnp.swapaxes(grad_logits_bf, 1, 2), w_gate.T), BF16)
        grad_gate_w = jnp.einsum('gsh,gse->he', x_loc, grad_logits_bf, preferred_element_type=F32)

        dot_sum = plain_sum + moe_sum
        local_stats = jnp.concatenate([jnp.sum(router_prob, axis=(0, 1)), dot_sum[None]])
        rows = hidden * experts // ep_size // 128
        own = grad_gate_w.reshape(ep_size, rows, 128)
        shared = jnp.zeros((8, 128), F32).at[0, :experts + 1].set(local_stats)
        packed = jnp.concatenate([own, jnp.broadcast_to(shared, (ep_size, 8, 128))], axis=1)
        packed = lax.all_to_all(after(packed, back[-1]), 'ep', 0, 0, tiled=True)
        total = jnp.sum(packed, axis=0)
        grad_gate_w = lax.all_to_all(jnp.broadcast_to(total[:rows], (ep_size, rows, 128)), 'ep', 0, 0, tiled=True).reshape(hidden, experts)
        global_stats = total[rows]
        mean_prob = global_stats[:experts] / tokens_all
        loss_value = global_stats[experts] / numel + ALPHA * experts * jnp.sum(frac_first * mean_prob)
        return loss_value, grad_x, grad_w_in, grad_w_out, grad_gate_w

    row_spec = P('ep', None, None)
    id_spec = P('ep', None)
    return jax.shard_map(layer, mesh=mesh, in_specs=(row_spec, row_spec, P(None, None), row_spec, row_spec, id_spec, id_spec, id_spec), out_specs=(P(), row_spec, row_spec, row_spec, P(None, None)), check_vma=False)
```
